16 devices in a mesh: dp: 2 (over y, z), sp: 8 (over x, core).
Axes of the slice: x: 4, y: 2, z: 1, core: 2. Of those that a mesh axis runs over, the one named last changes fastest.
The devices are a block of a 4x4x8 slice.
Arguments:
- x: bfloat16 [4096, 6144], P(('dp', 'sp')), parts along dimension 0
- gain: bfloat16 [6144], replicated
- wq: bfloat16 [6144, 6144], replicated
- wk: bfloat16 [6144, 1024], replicated
- wv: bfloat16 [6144, 1024], replicated
- wo: bfloat16 [6144, 6144], replicated
Outputs:
- output: bfloat16 [4096, 6144], P(('dp', 'sp')), parts along dimension 0
There are 2 independent parts. The reference program is written for one: setup_inputs(seed, part) draws one part's arguments, and reference() takes and returns one part's arrays. A program takes and returns all parts, laid end to end along the dimension named above; an argument that names none is the same for every part.
All inputs are finite; a program needn't handle non-finite values.
Results may differ from the reference program's by a relative error of at most 0.012.
Values are sent between devices in bfloat16 or wider.
A program may use at most 768 MiB of HBM per device.

```python
import jax
import jax.numpy as jnp
from jax import lax

ROWS = 2048
D = 6144
HEADS = 48
KV_HEADS = 8
HEAD = 128
THETA = 10000


def setup_inputs(seed: int = 0, part: int = 0) -> dict:
    kx, kn, kq, kk, kv, ko = jax.random.split(jax.random.key(seed), 6)

    def weights(key, rows, columns):
        return jax.random.normal(key, (rows, columns), jnp.float32) * rows**-0.5

    drawn = {
        "x": jax.random.normal(jax.random.fold_in(kx, part), (ROWS, D), jnp.float32),
        "gain": 1 + 0.1 * jax.random.normal(kn, (D,), jnp.float32),
        "wq": 2 * weights(kq, D, HEADS * HEAD),
        "wk": 2 * weights(kk, D, KV_HEADS * HEAD),
        "wv": 4 * weights(kv, D, KV_HEADS * HEAD),
        "wo": weights(ko, HEADS * HEAD, D),
    }
    return {k: v.astype(jnp.bfloat16) for k, v in drawn.items()}


def normed(x, gain):
    wide = x.astype(jnp.float32)
    scale = lax.rsqrt(jnp.mean(wide * wide, -1, keepdims=True) + 1e-6)
    return (wide * scale * gain.astype(jnp.float32)).astype(jnp.bfloat16)


def turned(t, place, theta):
    half = t.shape[-1] // 2
    angle = place.astype(jnp.float32)[:, None] * theta ** (-jnp.arange(half, dtype=jnp.float32) / half)
    cos, sin = jnp.cos(angle)[:, None], jnp.sin(angle)[:, None]
    a, b = t[..., :half].astype(jnp.float32), t[..., half:].astype(jnp.float32)
    return jnp.concatenate([a * cos - b * sin, b * cos + a * sin], -1).astype(jnp.bfloat16)


def matmul(a, w):
    return jnp.dot(a, w, preferred_element_type=jnp.float32).astype(jnp.bfloat16)


def einsum(form, a, b):
    return jnp.einsum(form, a.astype(jnp.float32), b.astype(jnp.float32))


def attention(q, k, v):
    scores = einsum("tgsd,ugd->gstu", q, k) * q.shape[-1] ** -0.5
    token = jnp.arange(q.shape[0])
    scores = jnp.where(token[:, None] >= token, scores, -jnp.inf)
    weights = jax.nn.softmax(scores, -1).astype(jnp.bfloat16)
    return einsum("gstu,ugd->tgsd", weights, v).astype(jnp.bfloat16)


def reference(x, gain, wq, wk, wv, wo):
    a, place = normed(x, gain), jnp.arange(ROWS)
    q = turned(matmul(a, wq).reshape(ROWS, HEADS, HEAD), place, THETA).reshape(ROWS, KV_HEADS, -1, HEAD)
    k = turned(matmul(a, wk).reshape(ROWS, KV_HEADS, HEAD), place, THETA)
    v = matmul(a, wv).reshape(ROWS, KV_HEADS, HEAD)
    seen = attention(q, k, v).reshape(ROWS, HEADS * HEAD)
    return (x.astype(jnp.float32) + jnp.dot(seen, wo, preferred_element_type=jnp.float32)).astype(jnp.bfloat16)
```

```python
import functools

import jax
import jax.numpy as jnp
from jax import lax
from jax.experimental import pallas as pl
from jax.experimental.pallas import tpu as pltpu
from jax.sharding import PartitionSpec as P

MESH = pl.DeviceIdType.MESH
HEAD = 128
THETA = 10000
CORES = 2
LOG2E = 1.4426950408889634
HIDDEN = -1e30
WIDE = 512
SLOTS = 3
ONES = 16
R1, R2, L1, L2, RF, LF = range(6)


def dot(a, b):
    return lax.dot_general(a, b, (((1,), (0,)), ((), ())), preferred_element_type=jnp.float32)


def turned(t, cos, sin):
    return t * cos + pltpu.roll(t, HEAD // 2, 1) * sin


def kernel(chips, x, gain, table, wq, wk, wv, wo, y, xv, av, wb, gv, tv, qt, kb, vb, acc, top, ob, orv, ys,
           xsem, tsem, wsem, asend, arecv, ksend, krecv, osend, orecv, ysem):
    own, width = xv.shape
    half_w = width // CORES
    kvh = kb.shape[2]
    heads = qt.shape[0]
    group = heads // kvh
    blocks_q, blocks_o = half_w // WIDE, width // WIDE
    me = lax.axis_index("sp")
    c, r = me // CORES, lax.rem(me, CORES)
    partner = c * CORES + 1 - r
    right = lax.rem(c + 1, chips) * CORES + r
    left = lax.rem(c + chips - 1, chips) * CORES + r

    def item(i, s):
        if isinstance(i, int) and i < 2:
            src = (wk, wv)[i].at[:, pl.ds(pl.multiple_of(r * WIDE, WIDE), WIDE)]
        elif isinstance(i, int):
            src = wq.at[:, pl.ds(pl.multiple_of(r * half_w + (i - 2) * WIDE, WIDE), WIDE)]
        return pltpu.make_async_copy(src, wb.at[s], wsem.at[s])

    def q_item(j):
        s = lax.rem(j + 2, SLOTS)
        return pltpu.make_async_copy(wq.at[:, pl.ds(pl.multiple_of(r * half_w + j * WIDE, WIDE), WIDE)], wb.at[s], wsem.at[s])

    def o_item(j):
        s = lax.rem(j + 2 + blocks_q, SLOTS)
        return pltpu.make_async_copy(wo.at[:, pl.ds(pl.multiple_of(j * WIDE, WIDE), WIDE)], wb.at[s], wsem.at[s])

    pieces = xsem.shape[0]
    rows = own // pieces
    x_copies = [pltpu.make_async_copy(x.at[pl.ds(i * rows, rows)], xv.at[pl.ds(i * rows, rows)], xsem.at[i]) for i in range(pieces)]
    g_copy = pltpu.make_async_copy(gain, gv, tsem.at[0])
    t_copy = pltpu.make_async_copy(table, tv, tsem.at[1])
    g_copy.start()
    for copy in x_copies:
        copy.start()
    item(0, 0).start()
    item(1, 1).start()
    t_copy.start()
    item(2, 2).start()

    barrier = pltpu.get_barrier_semaphore()
    for other in (partner, right, left):
        pl.semaphore_signal(barrier, inc=1, device_id={"sp": other}, device_id_type=MESH)

    def base(t):
        return pl.multiple_of(t * own, own)

    def a_copy(i):
        part = av.at[pl.ds(pl.multiple_of(base(r) + i * rows, rows), rows)]
        return pltpu.make_async_remote_copy(part, part, asend.at[i], arecv.at[i], device_id={"sp": partner}, device_id_type=MESH)

    g_copy.wait()
    step = 32
    for i in range(pieces):
        x_copies[i].wait()

        def norm(n, _):
            at = pl.multiple_of(i * rows + n * step, step)
            wide = xv[pl.ds(at, step), :].astype(jnp.float32)
            scale = lax.rsqrt(jnp.mean(wide * wide, -1, keepdims=True) + 1e-6)
            av[pl.ds(pl.multiple_of(base(r) + at, step), step), :] = (wide * scale * gv[...].astype(jnp.float32)).astype(jnp.bfloat16)

        lax.fori_loop(0, rows // step, norm, None)
        if i == 0:
            pl.semaphore_wait(barrier, 3)
        else:
            a_copy(i - 1).start()

    for t in range(kb.shape[0]):
        for b in range(CORES):
            for g in range(kvh):
                vb[t, b, g, HEAD:, :] = jnp.ones((ONES, own), jnp.bfloat16)
    a_copy(pieces - 1).start()

    def make_k(t):
        k = dot(av[pl.ds(base(t), own), :], wb[0]).astype(jnp.bfloat16).astype(jnp.float32)
        cos, sin = tv[0, pl.ds(base(t), own), :], tv[1, pl.ds(base(t), own), :]
        for g in range(kvh):
            kb[c, t, g] = turned(k[:, g * HEAD : (g + 1) * HEAD], cos, sin).astype(jnp.bfloat16)

    def make_v(t):
        v = dot(av[pl.ds(base(t), own), :], wb[1])
        for g in range(kvh):
            vb[c, t, g, :HEAD, :] = v[:, g * HEAD : (g + 1) * HEAD].T.astype(jnp.bfloat16)

    def kv_copies(message, chip, t, to):
        k, v = kb.at[chip, t], vb.at[chip, t, :, pl.ds(0, HEAD)]
        return [pltpu.make_async_remote_copy(part, part, ksend.at[message, i], krecv.at[message, i], device_id={"sp": to}, device_id_type=MESH)
                for i, part in enumerate((k, v))]

    second = lax.rem(c + 2, chips)
    before = lax.rem(c + chips - 1, chips)
    after = lax.rem(c + 1, chips)
    out = {R1: kv_copies(R1, c, r, right), R2: kv_copies(R2, c, 1 - r, right), L1: kv_copies(L1, c, r, left), L2: kv_copies(L2, c, 1 - r, left),
           RF: kv_copies(RF, before, r, right), LF: kv_copies(LF, after, 1 - r, left)}
    t_copy.wait()
    item(0, 0).wait()
    make_k(r)
    item(1, 1).wait()
    make_v(r)
    for m in (R1, L1):
        out[m][0].start()
    for i in range(pieces):
        a_copy(i).wait_recv()
    make_k(1 - r)
    for m in (R1, L1):
        out[m][1].start()
    q_item(jnp.int32(1)).start()
    make_v(1 - r)
    for m in (R2, L2):
        out[m][0].start()
    q_item(jnp.int32(2)).start()

    factor = HEAD**-0.5 * LOG2E
    per = WIDE // HEAD

    def make_q(j, _):
        q_item(j).wait()
        s = lax.rem(j + 2, SLOTS)
        q = dot(av[...], wb[s]).astype(jnp.bfloat16).astype(jnp.float32)
        for n in range(per):
            head = (turned(q[:, n * HEAD : (n + 1) * HEAD], tv[0], tv[1]) * factor).T.astype(jnp.bfloat16)
            for b in range(CORES):
                qt[j * per + n, b] = head[:, b * own : (b + 1) * own]

        @pl.when(j + SLOTS < blocks_q)
        def _():
            q_item(j + SLOTS).start()

        @pl.when(j + SLOTS >= blocks_q)
        def _():
            o_item(j + SLOTS - blocks_q).start()

        @pl.when(j == 0)
        def _():
            for m in (R2, L2):
                out[m][1].start()

        @pl.when(j == blocks_q - 2)
        def _():
            for copy in out[R1]:
                copy.wait_recv()
            for copy in out[RF]:
                copy.start()

    lax.fori_loop(0, blocks_q, make_q, None)
    for copy in out[L2]:
        copy.wait_recv()
    for copy in out[LF]:
        copy.start()

    seen = lax.broadcasted_iota(jnp.int32, (own, own), 0) <= lax.broadcasted_iota(jnp.int32, (own, own), 1)
    strips = [(n, b) for n in range(group) for b in range(CORES)]

    def attend(chip, g, diagonal):
        scores, weights, keeps = {}, {}, {}

        def score(i):
            n, b = strips[i]
            q = qt[g * group + n, b]
            scores[i] = [dot(kb[chip, t, g], q) for t in range(b + 1 if diagonal else CORES)]
            if diagonal:
                scores[i][b] = jnp.where(seen, scores[i][b], HIDDEN)

        def weigh(i):
            n, b = strips[i]
            at = (g * group + n) * CORES + b
            s = scores.pop(i)
            best = functools.reduce(jnp.maximum, [part.max(axis=0, keepdims=True) for part in s])
            if not diagonal:
                old = top[at]
                best = jnp.maximum(old, best)
                keeps[i] = jnp.exp2(old - best)
            top[at] = best
            weights[i] = [jnp.exp2(part - best).astype(jnp.bfloat16) for part in s]

        def add(i):
            n, b = strips[i]
            at = (g * group + n) * CORES + b
            new = functools.reduce(jnp.add, [dot(vb[chip, t, g], p) for t, p in enumerate(weights.pop(i))])
            acc[at] = new if diagonal else acc[at] * keeps.pop(i) + new

        lead, last = 3, len(strips)
        for i in range(lead):
            score(i)
        for i in range(last):
            weigh(i)
            if i + lead < last:
                score(i + lead)
            if i >= 1:
                add(i - 1)
        add(last - 1)

    lax.fori_loop(0, kvh, lambda g, _: attend(c, g, True), None)

    def others(n, _):
        phase, g = n // kvh, lax.rem(n, kvh)

        @pl.when(n == 0)
        def _():
            for copy in out[R2]:
                copy.wait_recv()

        @pl.when(n == kvh)
        def _():
            for copy in out[L1]:
                copy.wait_recv()

        @pl.when(n == 2 * kvh)
        def _():
            for m in (RF, LF):
                for copy in out[m]:
                    copy.wait_recv()

        chip = jnp.where(phase == 0, before, jnp.where(phase == 1, after, second))

        @pl.when(chip < c)
        def _():
            attend(chip, g, False)

    lax.fori_loop(0, 3 * kvh, others, None)

    def o_copy(g):
        cols = pl.ds(pl.multiple_of(g * group * HEAD, HEAD), group * HEAD)
        return pltpu.make_async_remote_copy(ob.at[1 - r, :, cols], orv.at[:, cols], osend.at[g], orecv.at[g],
                                            device_id={"sp": partner}, device_id_type=MESH)

    def finish(g, _):
        for b in range(CORES):
            for n in range(group):
                at = (g * group + n) * CORES + b
                o = (acc[at, :HEAD, :] * (1 / acc[at, HEAD : HEAD + 1, :])).T.astype(jnp.bfloat16)
                ob[b, :, pl.ds(pl.multiple_of((g * group + n) * HEAD, HEAD), HEAD)] = o

        @pl.when(g > 0)
        def _():
            o_copy(g - 1).start()

    lax.fori_loop(0, kvh, finish, None)
    o_copy(jnp.int32(kvh - 1)).start()
    for g in range(kvh):
        o_copy(jnp.int32(g)).wait_recv()

    def y_copy(j):
        return pltpu.make_async_copy(ys.at[lax.rem(j, 2)], y.at[:, pl.ds(pl.multiple_of(j * WIDE, WIDE), WIDE)], ysem.at[lax.rem(j, 2)])

    def project(j, _):
        o_item(j).wait()
        s = lax.rem(j + 2 + blocks_q, SLOTS)
        mine, theirs = pl.multiple_of(r * half_w, half_w), pl.multiple_of((1 - r) * half_w, half_w)
        new = dot(ob[r], wb[s, pl.ds(mine, half_w), :]) + dot(orv[...], wb[s, pl.ds(theirs, half_w), :])
        new = xv[:, pl.ds(pl.multiple_of(j * WIDE, WIDE), WIDE)].astype(jnp.float32) + new

        @pl.when(j >= 2)
        def _():
            y_copy(j - 2).wait()

        ys[lax.rem(j, 2)] = new.astype(jnp.bfloat16)
        y_copy(j).start()

        @pl.when(j + SLOTS < blocks_o)
        def _():
            o_item(j + SLOTS).start()

    lax.fori_loop(0, blocks_o, project, None)
    for j in (blocks_o - 2, blocks_o - 1):
        y_copy(jnp.int32(j)).wait()
    for i in range(pieces):
        a_copy(i).wait_send()
    for m in range(6):
        for copy in out[m]:
            copy.wait_send()
    for g in range(kvh):
        o_copy(jnp.int32(g)).wait_send()


def solution(mesh):
    chips = mesh.shape["sp"] // CORES

    def step(x, gain, wq, wk, wv, wo):
        own, width = x.shape
        shared = own * CORES
        kvh = wk.shape[1] // HEAD // CORES
        heads = wq.shape[1] // HEAD // CORES
        place = (lax.axis_index("sp") // CORES) * shared + jnp.arange(shared)
        half = HEAD // 2
        angle = place.astype(jnp.float32)[:, None] * THETA ** (-jnp.arange(half, dtype=jnp.float32) / half)
        cos, sin = jnp.cos(angle), jnp.sin(angle)
        table = jnp.stack([jnp.concatenate([cos, cos], -1), jnp.concatenate([-sin, sin], -1)])
        bf16, f32 = jnp.bfloat16, jnp.float32
        dma, pieces = pltpu.SemaphoreType.DMA, 4
        anywhere = pl.BlockSpec(memory_space=pl.ANY)
        return pl.pallas_call(
            functools.partial(kernel, chips),
            out_shape=jax.ShapeDtypeStruct((own, width), bf16),
            in_specs=[anywhere] * 7,
            out_specs=anywhere,
            scratch_shapes=[
                pltpu.VMEM((own, width), bf16),
                pltpu.VMEM((shared, width), bf16),
                pltpu.VMEM((SLOTS, width, WIDE), bf16),
                pltpu.VMEM((1, width), bf16),
                pltpu.VMEM((2, shared, HEAD), f32),
                pltpu.VMEM((heads, CORES, HEAD, own), bf16),
                pltpu.VMEM((chips, CORES, kvh, own, HEAD), bf16),
                pltpu.VMEM((chips, CORES, kvh, HEAD + ONES, own), bf16),
                pltpu.VMEM((heads * CORES, HEAD + ONES, own), f32),
                pltpu.VMEM((heads * CORES, 1, own), f32),
                pltpu.VMEM((CORES, own, heads * HEAD), bf16),
                pltpu.VMEM((own, heads * HEAD), bf16),
                pltpu.VMEM((2, own, WIDE), bf16),
                dma((pieces,)), dma((2,)), dma((SLOTS,)), dma((pieces,)), dma((pieces,)), dma((6, 2)), dma((6, 2)), dma((kvh,)), dma((kvh,)), dma((2,)),
            ],
            compiler_params=pltpu.CompilerParams(collective_id=0, has_side_effects=True, vmem_limit_bytes=67043328),
        )(x, gain[None], table, wq, wk, wv, wo)

    tokens, whole = P(("dp", "sp"), None), P(None, None)
    return jax.shard_map(
        step,
        mesh=mesh,
        in_specs=(tokens, P(None), whole, whole, whole, whole),
        out_specs=tokens,
        check_vma=False,
    )
```

```python
import functools
import math

import jax
import jax.numpy as jnp
from jax import lax
from jax.experimental import pallas as pl
from jax.experimental.pallas import tpu as pltpu
from jax.sharding import PartitionSpec as P

MESH = pl.DeviceIdType.MESH
HEAD = 128
THETA = 10000
CORES = 2
LOG2E = 1.4426950408889634
HIDDEN = -1e30
WIDE = 512
SLOTS = 3
ONES = 16
LEAD = 4
R1, R2, L1, L2, RF, LF = range(6)
SENDS = {R1: ({0, 2, 3}, {0, 1, 2}), R2: ({0, 3}, {0, 1, 2}), L1: ({1, 2}, {0}), L2: ({1, 2}, {0, 1}), RF: ({3}, {1, 2}), LF: ({1}, {0, 3})}


def dot(a, b):
    return lax.dot_general(a, b, (((1,), (0,)), ((), ())), preferred_element_type=jnp.float32)


def turned(t, cos, sin):
    return t * cos + pltpu.roll(t, HEAD // 2, 1) * sin


def among(chip, chips):
    return functools.reduce(jnp.logical_or, [chip == k for k in sorted(chips)])


def kernel(chips, x, gain, wq, wk, wv, wo, y, av, wb, gv, tv, qs_a, qs_b, qt, gq, gr, kb, vb, acc, top, of, go,
           xsem, gsem, wsem, asend, arecv, ksend, krecv, qsend, qrecv, osend, orecv, gsend, grecv):
    own, width = y.shape
    half_w = width // CORES
    kvh = kb.shape[2]
    heads = qt.shape[0]
    group = heads // kvh
    blocks_q, blocks_o = half_w // WIDE, width // WIDE
    me = lax.axis_index("sp")
    c, r = me // CORES, lax.rem(me, CORES)
    before, after, across = (lax.rem(c + k, chips) for k in (chips - 1, 1, 2))
    mate = chips - 1 - c
    late = c >= chips // 2
    partner, right, left = c * CORES + 1 - r, after * CORES + r, before * CORES + r

    def kv_item(i):
        return pltpu.make_async_copy((wk, wv)[i].at[:, pl.ds(pl.multiple_of(r * WIDE, WIDE), WIDE)], wb.at[i], wsem.at[i, 0])

    def q_item(j):
        s = lax.rem(j + 2, SLOTS)
        return pltpu.make_async_copy(wq.at[:, pl.ds(pl.multiple_of(r * half_w + j * WIDE, WIDE), WIDE)], wb.at[s], wsem.at[s, 0])

    slab = group * HEAD
    rest = half_w - slab
    many = half_w // slab

    def o_slot(j):
        return lax.rem(j + 2 + blocks_q, SLOTS)

    def o_copies(j):
        s = o_slot(j)
        cols = pl.ds(pl.multiple_of(j * WIDE, WIDE), WIDE)
        return [pltpu.make_async_copy(wo.at[pl.ds(h * half_w + slab, rest), cols], wb.at[s, pl.ds(h * rest, rest)], wsem.at[s, h])
                for h in range(CORES)]

    def p_copies(j):
        s = o_slot(j + blocks_o)
        return [pltpu.make_async_copy(wo.at[pl.ds(h * half_w, slab), pl.ds(pl.multiple_of((j * many + m) * WIDE, WIDE), WIDE)],
                                      wb.at[s, pl.ds((m * CORES + h) * slab, slab)], wsem.at[s, m * CORES + h])
                for m in range(many) for h in range(CORES)]

    def start(copies):
        for copy in copies:
            copy.start()

    def wait(copies):
        for copy in copies:
            copy.wait()

    pieces = xsem.shape[0]
    rows = own // pieces
    x_copies = [pltpu.make_async_copy(x.at[pl.ds(i * rows, rows)], y.at[pl.ds(i * rows, rows)], xsem.at[i]) for i in range(pieces)]
    g_copy = pltpu.make_async_copy(gain, gv, gsem)
    g_copy.start()
    for copy in x_copies:
        copy.start()
    kv_item(0).start()
    kv_item(1).start()
    q_item(jnp.int32(0)).start()

    barrier = pltpu.get_barrier_semaphore()
    for other in (partner, right, left, mate * CORES + 1 - r):
        pl.semaphore_signal(barrier, inc=1, device_id={"sp": other}, device_id_type=MESH)

    lane = lax.broadcasted_iota(jnp.int32, (own, HEAD), 1)
    rate = jnp.exp(lax.rem(lane, HEAD // 2).astype(jnp.float32) * (-math.log(THETA) / (HEAD // 2)))
    for t in range(CORES):
        angle = (c * (CORES * own) + t * own + lax.broadcasted_iota(jnp.int32, (own, HEAD), 0)).astype(jnp.float32) * rate
        sin = jnp.sin(angle)
        tv[0, t * own : (t + 1) * own, :] = jnp.cos(angle)
        tv[1, t * own : (t + 1) * own, :] = jnp.where(lane < HEAD // 2, -sin, sin)

    def base(t):
        return pl.multiple_of(t * own, own)

    def a_copy(i):
        part = av.at[pl.ds(pl.multiple_of(base(r) + i * rows, rows), rows)]
        return pltpu.make_async_remote_copy(part, part, asend.at[i], arecv.at[i], device_id={"sp": partner}, device_id_type=MESH)

    g_copy.wait()
    step = 32
    for i in range(pieces):
        x_copies[i].wait()

        def norm(n, _):
            at = pl.multiple_of(i * rows + n * step, step)
            wide = y[pl.ds(at, step), :].astype(jnp.float32)
            scale = lax.rsqrt(jnp.mean(wide * wide, -1, keepdims=True) + 1e-6)
            gains = gv[...].astype(jnp.float32).reshape(1, width)
            av[pl.ds(pl.multiple_of(base(r) + at, step), step), :] = (wide * scale * gains).astype(jnp.bfloat16)

        lax.fori_loop(0, rows // step, norm, None)
        if i == 0:
            pl.semaphore_wait(barrier, 4)
        else:
            a_copy(i - 1).start()

    for t in range(kb.shape[0]):
        for b in range(CORES):
            for g in range(kvh):
                vb[t, b, g, HEAD:, :] = jnp.ones((ONES, own), jnp.bfloat16)
    qs_b[...] = jnp.zeros_like(qs_b)
    a_copy(pieces - 1).start()

    def make_k(t):
        k = dot(av[pl.ds(base(t), own), :], wb[0]).astype(jnp.bfloat16).astype(jnp.float32)
        cos, sin = tv[0, pl.ds(base(t), own), :], tv[1, pl.ds(base(t), own), :]
        for g in range(kvh):
            kb[c, t, g] = turned(k[:, g * HEAD : (g + 1) * HEAD], cos, sin).astype(jnp.bfloat16)

    def make_v(t):
        v = dot(av[pl.ds(base(t), own), :], wb[1])
        for g in range(kvh):
            vb[c, t, g, :HEAD, :] = v[:, g * HEAD : (g + 1) * HEAD].T.astype(jnp.bfloat16)

    def kv_copies(message, chip, t, to):
        copies = []
        for p, (first, count) in enumerate(((0, 1), (1, kvh - 1))):
            refs = kb.at[chip, t, pl.ds(first, count)], vb.at[chip, t, pl.ds(first, count), pl.ds(0, HEAD)]
            copies.append([pltpu.make_async_remote_copy(ref, ref, ksend.at[message, p, i], krecv.at[message, p, i], device_id={"sp": to},
                                                        device_id_type=MESH) for i, ref in enumerate(refs)])
        return copies

    out = {R1: kv_copies(R1, c, r, right), R2: kv_copies(R2, c, 1 - r, right), L1: kv_copies(L1, c, r, left), L2: kv_copies(L2, c, 1 - r, left),
           RF: kv_copies(RF, before, r, right), LF: kv_copies(LF, after, 1 - r, left)}

    def send(message, part, which=(0, 1)):
        @pl.when(among(c, SENDS[message][part]))
        def _():
            for i in which:
                out[message][part][i].start()

    def arrived(message, part):
        @pl.when(among(before if message in (R1, R2, RF) else after, SENDS[message][part]))
        def _():
            for copy in out[message][part]:
                copy.wait_recv()

    kv_item(0).wait()
    kv_item(1).wait()
    make_k(r)
    make_v(r)
    for part in range(2):
        for m in (R1, L1):
            send(m, part, (0,))
    for i in range(pieces):
        a_copy(i).wait_recv()
    make_k(1 - r)
    q_item(jnp.int32(1)).start()
    make_v(1 - r)
    q_item(jnp.int32(2)).start()
    for part in range(2):
        for m in (R1, L1):
            send(m, part, (1,))

    factor = HEAD**-0.5 * LOG2E
    per = WIDE // HEAD

    def split(q):
        wide = q.astype(jnp.float32) * factor
        high = wide.astype(jnp.bfloat16)
        return high, (wide - high.astype(jnp.float32)).astype(jnp.bfloat16)

    def turn_q(j, made):
        for n in range(per):
            q = turned(made[:, n * HEAD : (n + 1) * HEAD].astype(jnp.float32), tv[0], tv[1]).astype(jnp.bfloat16).T
            high, low = split(q)
            for b in range(CORES):
                cols = slice(b * own, (b + 1) * own)
                gq[jnp.minimum(j * per + n, gq.shape[0] - 1), b] = q[:, cols]
                qt[j * per + n, b, :HEAD, :] = high[:, cols]
                qt[j * per + n, b, HEAD:, :] = low[:, cols]

    def refill(j):
        @pl.when(j + SLOTS < blocks_q)
        def _():
            q_item(j + SLOTS).start()

        @pl.when(j + SLOTS >= blocks_q)
        def _():
            start(o_copies(j + SLOTS - blocks_q))

    q_copy = pltpu.make_async_remote_copy(gq.at[pl.ds(0, group)], gr, qsend, qrecv, device_id={"sp": mate * CORES + r}, device_id_type=MESH)

    def make_q(i, _):
        j = 2 * i
        q_item(j).wait()
        qs_a[...] = dot(av[...], wb[lax.rem(j + 2, SLOTS)]).astype(jnp.bfloat16)
        turn_q(jnp.maximum(j - 1, 0), qs_b)
        refill(j)

        @pl.when(i == 0)
        def _():
            for part in range(2):
                for m in (R2, L2):
                    send(m, part)

        @pl.when(i == 1)
        def _():
            arrived(R1, 0)
            send(RF, 0)
            arrived(L2, 0)
            send(LF, 0)

        q_item(j + 1).wait()
        qs_b[...] = dot(av[...], wb[lax.rem(j + 3, SLOTS)]).astype(jnp.bfloat16)
        turn_q(j, qs_a)
        refill(j + 1)

        @pl.when((i == 1) & late)
        def _():
            q_copy.start()

        @pl.when(i == 1)
        def _():
            arrived(R1, 1)
            send(RF, 1)

    lax.fori_loop(0, blocks_q // 2, make_q, None)
    turn_q(blocks_q - 1, qs_b)
    arrived(L2, 1)
    send(LF, 1)

    seen = lax.broadcasted_iota(jnp.int32, (own, own), 0) <= lax.broadcasted_iota(jnp.int32, (own, own), 1)
    strips = [(n, b) for n in range(group) for b in range(CORES)]

    def strip(g, n, b):
        return pl.ds(pl.multiple_of(((g * group + n) * CORES + b) * (HEAD + ONES), ONES), HEAD + ONES)

    def attend(chip, g, diagonal):
        scores, weights, keeps = {}, {}, {}

        def keys(t):
            k = kb[chip, t, g]
            return jnp.concatenate([k, k], axis=1)

        def score(i):
            n, b = strips[i]
            q = qt[g * group + n, b]
            scores[i] = [dot(keys(t), q) for t in range(b + 1 if diagonal else CORES)]
            if diagonal:
                scores[i][b] = jnp.where(seen, scores[i][b], HIDDEN)

        def weigh(i):
            n, b = strips[i]
            at = (g * group + n) * CORES + b
            s = scores.pop(i)
            best = functools.reduce(jnp.maximum, [x.max(axis=0, keepdims=True) for x in s])
            if not diagonal:
                old = top[at]
                best = jnp.maximum(old, best)
                keeps[i] = jnp.exp2(old - best)
            top[at] = best
            weights[i] = [jnp.exp2(x - best).astype(jnp.bfloat16) for x in s]

        def add(i):
            n, b = strips[i]
            at = strip(g, n, b)
            new = functools.reduce(jnp.add, [dot(vb[chip, t, g], p) for t, p in enumerate(weights.pop(i))])
            acc[at, :] = new if diagonal else acc[at, :] * keeps.pop(i) + new

        last = len(strips)
        for i in range(LEAD):
            score(i)
        for i in range(last):
            weigh(i)
            if i + LEAD < last:
                score(i + LEAD)
            if i >= 1:
                add(i - 1)
        add(last - 1)

    def result(g, n, b):
        mixed = acc[strip(g, n, b), :]
        return (mixed[:HEAD] * (1 / mixed[HEAD : HEAD + 1])).astype(jnp.bfloat16).T

    first = jnp.where(late, 1, 0)
    lax.fori_loop(first, kvh, lambda g, _: attend(c, g, True), None)

    def others(n, _):
        phase, g = n // kvh, lax.rem(n, kvh)
        for at, messages in enumerate(((R2,), (L1,), (RF, LF))):

            @pl.when(n == at * kvh)
            def _():
                for m in messages:
                    for part in range(2):
                        arrived(m, part)

        chip = jnp.where(phase == 0, before, jnp.where(phase == 1, after, across))

        @pl.when((chip < c) & (g >= first))
        def _():
            attend(chip, g, False)

    lax.fori_loop(0, 3 * kvh, others, None)

    def o_copy(g):
        cols = pl.ds(pl.multiple_of(g * group * HEAD, HEAD), group * HEAD)
        return pltpu.make_async_remote_copy(of.at[CORES, :, cols], of.at[r, :, cols], osend.at[g], orecv.at[g],
                                            device_id={"sp": partner}, device_id_type=MESH)

    def finish(g, _):
        for b in range(CORES):
            to = jnp.where(r == b, b, CORES)
            for n in range(group):
                of[to, :, pl.ds(pl.multiple_of((g * group + n) * HEAD, HEAD), HEAD)] = result(g, n, b)

        @pl.when(g > first)
        def _():
            o_copy(g - 1).start()

    lax.fori_loop(first, kvh, finish, None)

    def g_copies():
        return [pltpu.make_async_remote_copy(go.at[b], of.at[r, :, pl.ds(0, group * HEAD)], gsend.at[b], grecv.at[r],
                                             device_id={"sp": mate * CORES + b}, device_id_type=MESH) for b in range(CORES)]

    @pl.when(jnp.logical_not(late))
    def _():
        q_copy.wait_recv()
        for n in range(group):
            for b in range(CORES):
                high, low = split(gr[n, b])
                qt[n, b, :HEAD, :] = high
                qt[n, b, HEAD:, :] = low
        o_copy(jnp.int32(kvh - 1)).start()
        attend(mate, 0, True)
        lax.fori_loop(0, mate, lambda t, _: attend(t, 0, False), None)
        for b in range(CORES):
            for n in range(group):
                go[b, :, n * HEAD : (n + 1) * HEAD] = result(0, n, b)
        for copy in g_copies():
            copy.start()

    @pl.when(late)
    def _():
        o_copy(jnp.int32(kvh - 1)).start()

    for g in range(1, kvh):
        o_copy(jnp.int32(g)).wait_recv()

    def halves(j):
        return [(pl.ds(pl.multiple_of((j * (WIDE // own) + k) * own, own), own), slice(k * own, (k + 1) * own)) for k in range(WIDE // own)]

    def project(j, _):
        wait(o_copies(j))
        s = o_slot(j)
        new = dot(of[0, :, slab:], wb[s, :rest, :]) + dot(of[1, :, slab:], wb[s, rest : CORES * rest, :])
        for to, cols in halves(j):
            acc[to, :] = new[:, cols]

        @pl.when(j + SLOTS < blocks_o)
        def _():
            start(o_copies(j + SLOTS))

        @pl.when(j + SLOTS >= blocks_o)
        def _():
            start(p_copies(j + SLOTS - blocks_o))

    lax.fori_loop(0, blocks_o, project, None)

    @pl.when(late)
    def _():
        for h in range(CORES):
            come = of.at[h, :, pl.ds(0, slab)]
            pltpu.make_async_copy(come, come, grecv.at[h]).wait()

    @pl.when(jnp.logical_not(late))
    def _():
        o_copy(jnp.int32(0)).wait_recv()

    def project_rest(j, _):
        wait(p_copies(j))
        s = o_slot(j + blocks_o)
        for m in range(many):
            new = [dot(of[h, :, :slab], wb[s, (m * CORES + h) * slab : (m * CORES + h + 1) * slab, :]) for h in range(CORES)]
            new = new[0] + new[1]
            at = j * many + m
            cols = pl.ds(pl.multiple_of(at * WIDE, WIDE), WIDE)
            before = jnp.concatenate([acc[to, :] for to, _ in halves(at)], axis=1)
            y[:, cols] = (y[:, cols].astype(jnp.float32) + (before + new)).astype(jnp.bfloat16)

        @pl.when(j + SLOTS < blocks_o // many)
        def _():
            start(p_copies(j + SLOTS))

    lax.fori_loop(0, blocks_o // many, project_rest, None)
    for i in range(pieces):
        a_copy(i).wait_send()
    for m in range(6):
        for part in range(2):

            @pl.when(among(c, SENDS[m][part]))
            def _():
                for copy in out[m][part]:
                    copy.wait_send()

    for g in range(1, kvh):
        o_copy(jnp.int32(g)).wait_send()

    @pl.when(late)
    def _():
        q_copy.wait_send()

    @pl.when(jnp.logical_not(late))
    def _():
        o_copy(jnp.int32(0)).wait_send()
        for copy in g_copies():
            copy.wait_send()


def solution(mesh):
    chips = mesh.shape["sp"] // CORES

    def step(x, gain, wq, wk, wv, wo):
        own, width = x.shape
        shared = own * CORES
        kvh = wk.shape[1] // HEAD // CORES
        heads = wq.shape[1] // HEAD // CORES
        group = heads // kvh
        bf16, f32 = jnp.bfloat16, jnp.float32
        dma, pieces = pltpu.SemaphoreType.DMA, 4
        return pl.pallas_call(
            functools.partial(kernel, chips),
            out_shape=pltpu.VMEM((own, width), bf16),
            in_specs=[pl.BlockSpec(memory_space=pl.ANY)] * 6,
            out_specs=pl.BlockSpec(memory_space=pltpu.VMEM),
            scratch_shapes=[
                pltpu.VMEM((shared, width), bf16),
                pltpu.VMEM((SLOTS, width, WIDE), bf16),
                pltpu.VMEM((width,), bf16),
                pltpu.VMEM((2, shared, HEAD), f32),
                pltpu.VMEM((shared, WIDE), bf16),
                pltpu.VMEM((shared, WIDE), bf16),
                pltpu.VMEM((heads, CORES, 2 * HEAD, own), bf16),
                pltpu.VMEM((group + 2, CORES, HEAD, own), bf16),
                pltpu.VMEM((group, CORES, HEAD, own), bf16),
                pltpu.VMEM((chips, CORES, kvh, own, HEAD), bf16),
                pltpu.VMEM((chips, CORES, kvh, HEAD + ONES, own), bf16),
                pltpu.VMEM((heads * CORES * (HEAD + ONES), own), f32),
                pltpu.VMEM((heads * CORES, 1, own), f32),
                pltpu.VMEM((CORES + 1, own, heads * HEAD), bf16),
                pltpu.VMEM((CORES, own, group * HEAD), bf16),
                dma((pieces,)), dma, dma((SLOTS, 2 * kvh)), dma((pieces,)), dma((pieces,)), dma((6, 2, 2)), dma((6, 2, 2)), dma, dma, dma((kvh,)), dma((kvh,)),
                dma((CORES,)), dma((CORES,)),
            ],
            compiler_params=pltpu.CompilerParams(collective_id=0, has_side_effects=True, vmem_limit_bytes=60 * 2**20),
        )(x, gain, wq, wk, wv, wo)

    tokens, whole = P(("dp", "sp"), None), P(None, None)
    return jax.shard_map(
        step,
        mesh=mesh,
        in_specs=(tokens, P(None), whole, whole, whole, whole),
        out_specs=tokens,
        check_vma=False,
    )
```

```python
import functools
import math

import jax
import jax.numpy as jnp
from jax import lax
from jax.experimental import pallas as pl
from jax.experimental.pallas import tpu as pltpu
from jax.sharding import PartitionSpec as P

MESH = pl.DeviceIdType.MESH
HEAD = 128
THETA = 10000
CORES = 2
LOG2E = 1.4426950408889634
HIDDEN = -1e30
WIDE = 512
SLOTS, O_SLOTS = 3, 4
ONES = 16
LEAD = 4
R1, R2, L1, L2, RF, LF = range(6)
SENDS = {R1: ({0, 2, 3}, {0, 1, 2}), R2: ({0, 3}, {0, 1, 2}), L1: ({1, 2}, {0}), L2: ({1, 2}, {0, 1}), RF: ({3}, {1, 2}), LF: ({1}, {0, 3})}


def dot(a, b):
    return lax.dot_general(a, b, (((1,), (0,)), ((), ())), preferred_element_type=jnp.float32)


def turned(t, cos, sin):
    return t * cos + pltpu.roll(t, HEAD // 2, 1) * sin


def among(chip, chips):
    return functools.reduce(jnp.logical_or, [chip == k for k in sorted(chips)])


def kernel(chips, x, gain, wq, wk, wv, wo, y, av, wb, gv, tv, qs_a, qs_b, qt, gq, gr, kb, vb, acc, top, of, go,
           xsem, gsem, wsem, asend, arecv, ksend, krecv, qsend, qrecv, osend, orecv, gsend, grecv):
    own, width = y.shape
    half_w = width // CORES
    kvh = kb.shape[2]
    heads = qt.shape[0]
    group = heads // kvh
    blocks_q, blocks_o = half_w // WIDE, width // WIDE
    me = lax.axis_index("sp")
    c, r = me // CORES, lax.rem(me, CORES)
    before, after, across = (lax.rem(c + k, chips) for k in (chips - 1, 1, 2))
    mate = chips - 1 - c
    late = c >= chips // 2
    partner, right, left = c * CORES + 1 - r, after * CORES + r, before * CORES + r

    def slot(s):
        return pl.ds(pl.multiple_of(s * width, width), width)

    def kv_item(i):
        return pltpu.make_async_copy((wk, wv)[i].at[:, pl.ds(pl.multiple_of(r * WIDE, WIDE), WIDE)], wb.at[slot(i)], wsem.at[i, 0])

    def q_slot(j):
        return lax.rem(j + 2, SLOTS)

    def q_item(j):
        s = q_slot(j)
        return pltpu.make_async_copy(wq.at[:, pl.ds(pl.multiple_of(r * half_w + j * WIDE, WIDE), WIDE)], wb.at[slot(s)], wsem.at[s, 0])

    slab = group * HEAD
    rest = half_w - slab
    many = rest // slab
    rows_o = CORES * rest

    def o_rows(j, first, count):
        return pl.ds(pl.multiple_of(lax.rem(j, O_SLOTS) * rows_o + first, slab), count)

    def o_copies(j):
        cols = pl.ds(pl.multiple_of(j * WIDE, WIDE), WIDE)
        return [pltpu.make_async_copy(wo.at[pl.ds(h * half_w + slab, rest), cols], wb.at[o_rows(j, h * rest, rest)], wsem.at[lax.rem(j, O_SLOTS), h])
                for h in range(CORES)]

    def p_copies(j):
        return [pltpu.make_async_copy(wo.at[pl.ds(h * half_w, slab), pl.ds(pl.multiple_of((j * many + m) * WIDE, WIDE), WIDE)],
                                      wb.at[o_rows(j, (m * CORES + h) * slab, slab)], wsem.at[lax.rem(j, O_SLOTS), m * CORES + h])
                for m in range(many) for h in range(CORES)]

    def start(copies):
        for copy in copies:
            copy.start()

    def wait(copies):
        for copy in copies:
            copy.wait()

    pieces = xsem.shape[0]
    rows = own // pieces
    x_copies = [pltpu.make_async_copy(x.at[pl.ds(i * rows, rows)], y.at[pl.ds(i * rows, rows)], xsem.at[i]) for i in range(pieces)]
    g_copy = pltpu.make_async_copy(gain, gv, gsem)
    g_copy.start()
    for copy in x_copies:
        copy.start()
    kv_item(0).start()

    barrier = pltpu.get_barrier_semaphore()
    for other in (partner, right, left, mate * CORES + 1 - r):
        pl.semaphore_signal(barrier, inc=1, device_id={"sp": other}, device_id_type=MESH)

    lane = lax.broadcasted_iota(jnp.int32, (own, HEAD), 1)
    rate = jnp.exp(lax.rem(lane, HEAD // 2).astype(jnp.float32) * (-math.log(THETA) / (HEAD // 2)))
    for t in range(CORES):
        angle = (c * (CORES * own) + t * own + lax.broadcasted_iota(jnp.int32, (own, HEAD), 0)).astype(jnp.float32) * rate
        sin = jnp.sin(angle)
        tv[0, t * own : (t + 1) * own, :] = jnp.cos(angle)
        tv[1, t * own : (t + 1) * own, :] = jnp.where(lane < HEAD // 2, -sin, sin)

    def base(t):
        return pl.multiple_of(t * own, own)

    def a_copy(i):
        part = av.at[pl.ds(pl.multiple_of(base(r) + i * rows, rows), rows)]
        return pltpu.make_async_remote_copy(part, part, asend.at[i], arecv.at[i], device_id={"sp": partner}, device_id_type=MESH)

    g_copy.wait()
    step = 32
    for i in range(pieces):
        x_copies[i].wait()

        def norm(n, _):
            at = pl.multiple_of(i * rows + n * step, step)
            wide = y[pl.ds(at, step), :].astype(jnp.float32)
            scale = lax.rsqrt(jnp.mean(wide * wide, -1, keepdims=True) + 1e-6)
            gains = gv[...].astype(jnp.float32).reshape(1, width)
            av[pl.ds(pl.multiple_of(base(r) + at, step), step), :] = (wide * scale * gains).astype(jnp.bfloat16)

        lax.fori_loop(0, rows // step, norm, None)
        if i == 0:
            kv_item(1).start()
            pl.semaphore_wait(barrier, 4)
        else:
            a_copy(i - 1).start()

    for t in range(kb.shape[0]):
        for b in range(CORES):
            for g in range(kvh):
                vb[t, b, g, HEAD:, :] = jnp.ones((ONES, own), jnp.bfloat16)
    qs_b[...] = jnp.zeros_like(qs_b)
    a_copy(pieces - 1).start()

    def make_k(t):
        k = dot(av[pl.ds(base(t), own), :], wb[slot(0), :]).astype(jnp.bfloat16).astype(jnp.float32)
        cos, sin = tv[0, pl.ds(base(t), own), :], tv[1, pl.ds(base(t), own), :]
        for g in range(kvh):
            kb[c, t, g] = turned(k[:, g * HEAD : (g + 1) * HEAD], cos, sin).astype(jnp.bfloat16)

    def make_v(t):
        v = dot(av[pl.ds(base(t), own), :], wb[slot(1), :])
        for g in range(kvh):
            vb[c, t, g, :HEAD, :] = v[:, g * HEAD : (g + 1) * HEAD].T.astype(jnp.bfloat16)

    def kv_copies(message, chip, t, to):
        copies = []
        for p, (first, count) in enumerate(((0, 1), (1, kvh - 1))):
            refs = kb.at[chip, t, pl.ds(first, count)], vb.at[chip, t, pl.ds(first, count), pl.ds(0, HEAD)]
            copies.append([pltpu.make_async_remote_copy(ref, ref, ksend.at[message, p, i], krecv.at[message, p, i], device_id={"sp": to},
                                                        device_id_type=MESH) for i, ref in enumerate(refs)])
        return copies

    out = {R1: kv_copies(R1, c, r, right), R2: kv_copies(R2, c, 1 - r, right), L1: kv_copies(L1, c, r, left), L2: kv_copies(L2, c, 1 - r, left),
           RF: kv_copies(RF, before, r, right), LF: kv_copies(LF, after, 1 - r, left)}

    def send(message, part, which=(0, 1)):
        @pl.when(among(c, SENDS[message][part]))
        def _():
            for i in which:
                out[message][part][i].start()

    def arrived(message, part):
        @pl.when(among(before if message in (R1, R2, RF) else after, SENDS[message][part]))
        def _():
            for copy in out[message][part]:
                copy.wait_recv()

    kv_item(0).wait()
    make_k(r)
    kv_item(1).wait()
    q_item(jnp.int32(0)).start()
    make_v(r)
    for part in range(2):
        for m in (R1, L1):
            send(m, part, (0,))
    for i in range(pieces):
        a_copy(i).wait_recv()
    make_k(1 - r)
    q_item(jnp.int32(1)).start()
    make_v(1 - r)
    q_item(jnp.int32(2)).start()
    for part in range(2):
        for m in (R1, L1):
            send(m, part, (1,))

    factor = HEAD**-0.5 * LOG2E
    per = WIDE // HEAD

    def split(q):
        wide = q.astype(jnp.float32) * factor
        high = wide.astype(jnp.bfloat16)
        return high, (wide - high.astype(jnp.float32)).astype(jnp.bfloat16)

    def turn_q(j, made):
        for n in range(per):
            q = turned(made[:, n * HEAD : (n + 1) * HEAD].astype(jnp.float32), tv[0], tv[1]).astype(jnp.bfloat16).T
            high, low = split(q)
            for b in range(CORES):
                cols = slice(b * own, (b + 1) * own)
                gq[jnp.minimum(j * per + n, gq.shape[0] - 1), b] = q[:, cols]
                qt[j * per + n, b, :HEAD, :] = high[:, cols]
                qt[j * per + n, b, HEAD:, :] = low[:, cols]

    def refill(j):
        @pl.when(j + SLOTS < blocks_q)
        def _():
            q_item(j + SLOTS).start()

        for back, items in ((3, (3,)), (2, (0,)), (1, (1, 2))):

            @pl.when(j == blocks_q - back)
            def _():
                for k in items:
                    start(o_copies(jnp.int32(k)))

    q_copy = pltpu.make_async_remote_copy(gq.at[pl.ds(0, group)], gr, qsend, qrecv, device_id={"sp": mate * CORES + r}, device_id_type=MESH)

    def make_q(i, _):
        j = 2 * i
        q_item(j).wait()
        qs_a[...] = dot(av[...], wb[slot(q_slot(j)), :]).astype(jnp.bfloat16)
        turn_q(jnp.maximum(j - 1, 0), qs_b)
        refill(j)

        @pl.when(i == 0)
        def _():
            for part in range(2):
                for m in (R2, L2):
                    send(m, part)

        @pl.when(i == 1)
        def _():
            arrived(R1, 0)
            send(RF, 0)
            arrived(L2, 0)
            send(LF, 0)

        @pl.when((i == 1) & late)
        def _():
            q_copy.start()

        q_item(j + 1).wait()
        qs_b[...] = dot(av[...], wb[slot(q_slot(j + 1)), :]).astype(jnp.bfloat16)
        turn_q(j, qs_a)
        refill(j + 1)

        @pl.when(i == 1)
        def _():
            arrived(R1, 1)
            send(RF, 1)

    lax.fori_loop(0, blocks_q // 2, make_q, None)
    turn_q(blocks_q - 1, qs_b)
    arrived(L2, 1)
    send(LF, 1)

    seen = lax.broadcasted_iota(jnp.int32, (own, own), 0) <= lax.broadcasted_iota(jnp.int32, (own, own), 1)
    strips = [(n, b) for n in range(group) for b in range(CORES)]

    def strip(g, n, b):
        return pl.ds(pl.multiple_of(((g * group + n) * CORES + b) * (HEAD + ONES), ONES), HEAD + ONES)

    def attend(chip, g, diagonal):
        scores, weights, keeps = {}, {}, {}

        def keys(t):
            k = kb[chip, t, g]
            return jnp.concatenate([k, k], axis=1)

        def score(i):
            n, b = strips[i]
            q = qt[g * group + n, b]
            scores[i] = [dot(keys(t), q) for t in range(b + 1 if diagonal else CORES)]
            if diagonal:
                scores[i][b] = jnp.where(seen, scores[i][b], HIDDEN)

        def weigh(i):
            n, b = strips[i]
            at = (g * group + n) * CORES + b
            s = scores.pop(i)
            best = functools.reduce(jnp.maximum, [x.max(axis=0, keepdims=True) for x in s])
            if not diagonal:
                old = top[at]
                best = jnp.maximum(old, best)
                keeps[i] = jnp.exp2(old - best)
            top[at] = best
            weights[i] = [jnp.exp2(x - best).astype(jnp.bfloat16) for x in s]

        def add(i):
            n, b = strips[i]
            at = strip(g, n, b)
            new = functools.reduce(jnp.add, [dot(vb[chip, t, g], p) for t, p in enumerate(weights.pop(i))])
            acc[at, :] = new if diagonal else acc[at, :] * keeps.pop(i) + new

        last = len(strips)
        for i in range(LEAD):
            score(i)
        for i in range(last):
            weigh(i)
            if i + LEAD < last:
                score(i + LEAD)
            if i >= 1:
                add(i - 1)
        add(last - 1)

    def result(g, n, b):
        mixed = acc[strip(g, n, b), :]
        return (mixed[:HEAD] * (1 / mixed[HEAD : HEAD + 1])).astype(jnp.bfloat16).T

    first = jnp.where(late, 1, 0)
    lax.fori_loop(first, kvh, lambda g, _: attend(c, g, True), None)

    def o_copy(g):
        cols = pl.ds(pl.multiple_of(g * group * HEAD, HEAD), group * HEAD)
        return pltpu.make_async_remote_copy(of.at[CORES, :, cols], of.at[r, :, cols], osend.at[g], orecv.at[g],
                                            device_id={"sp": partner}, device_id_type=MESH)

    def finish(g, _):
        for b in range(CORES):
            to = jnp.where(r == b, b, CORES)
            for n in range(group):
                of[to, :, pl.ds(pl.multiple_of((g * group + n) * HEAD, HEAD), HEAD)] = result(g, n, b)

        @pl.when(g > first)
        def _():
            o_copy(g - 1).start()

    def phase(n, _):
        for at, messages in enumerate(((R2,), (L1,), (RF, LF))):

            @pl.when(n == at)
            def _():
                for m in messages:
                    for part in range(2):
                        arrived(m, part)

        chip = jnp.where(n == 0, before, jnp.where(n == 1, after, across))

        def others(g, _):
            attend(chip, g, False)

            @pl.when((n == 2) & late)
            def _():
                finish(g, None)

        lax.fori_loop(jnp.where(chip < c, first, kvh), kvh, others, None)

    lax.fori_loop(0, 3, phase, None)
    lax.fori_loop(jnp.where(late, kvh, first), kvh, finish, None)

    def g_copies():
        return [pltpu.make_async_remote_copy(go.at[b], of.at[r, :, pl.ds(0, group * HEAD)], gsend.at[b], grecv.at[r],
                                             device_id={"sp": mate * CORES + b}, device_id_type=MESH) for b in range(CORES)]

    @pl.when(jnp.logical_not(late))
    def _():
        q_copy.wait_recv()
        for n in range(group):
            for b in range(CORES):
                high, low = split(gr[n, b])
                qt[n, b, :HEAD, :] = high
                qt[n, b, HEAD:, :] = low
        o_copy(jnp.int32(kvh - 1)).start()
        attend(mate, 0, True)
        lax.fori_loop(0, mate, lambda t, _: attend(t, 0, False), None)
        for b in range(CORES):
            for n in range(group):
                go[b, :, n * HEAD : (n + 1) * HEAD] = result(0, n, b)
        for copy in g_copies():
            copy.start()

    @pl.when(late)
    def _():
        o_copy(jnp.int32(kvh - 1)).start()

    def halves(j):
        return [(pl.ds(pl.multiple_of((j * (WIDE // own) + k) * own, own), own), slice(k * own, (k + 1) * own)) for k in range(WIDE // own)]

    def keep(j, new, more=False):
        for to, cols in halves(j):
            acc[to, :] = acc[to, :] + new[:, cols] if more else new[:, cols]

    def of_core(h, j):
        return dot(of[h, :, slab:], wb[o_rows(j, h * rest, rest), :])

    early = [jnp.int32(k) for k in range(2)]
    for j in early:
        wait(o_copies(j))
    for j in early:
        keep(j, of_core(r, j))
    for g in range(1, kvh):
        o_copy(jnp.int32(g)).wait_recv()
    for j in early:
        keep(j, of_core(1 - r, j), True)
        start(o_copies(j + O_SLOTS))

    def project(after):
        def two(i, _):
            for j in (2 * i, 2 * i + 1):
                wait(o_copies(j))
            for j in (2 * i, 2 * i + 1):
                keep(j, of_core(0, j) + of_core(1, j))
                start(after(j + O_SLOTS))

        return two

    lax.fori_loop(1, (blocks_o - O_SLOTS) // 2, project(o_copies), None)
    lax.fori_loop((blocks_o - O_SLOTS) // 2, blocks_o // 2, project(lambda j: p_copies(j - blocks_o)), None)

    @pl.when(late)
    def _():
        for h in range(CORES):
            come = of.at[h, :, pl.ds(0, slab)]
            pltpu.make_async_copy(come, come, grecv.at[h]).wait()

    @pl.when(jnp.logical_not(late))
    def _():
        o_copy(jnp.int32(0)).wait_recv()

    def project_rest(i, _):
        for j in (2 * i, 2 * i + 1):
            wait(p_copies(j))
        for j in (2 * i, 2 * i + 1):
            for m in range(many):
                new = [dot(of[h, :, :slab], wb[o_rows(j, (m * CORES + h) * slab, slab), :]) for h in range(CORES)]
                at = j * many + m
                cols = pl.ds(pl.multiple_of(at * WIDE, WIDE), WIDE)
                most = jnp.concatenate([acc[to, :] for to, _ in halves(at)], axis=1)
                y[:, cols] = (y[:, cols].astype(jnp.float32) + (most + (new[0] + new[1]))).astype(jnp.bfloat16)

    lax.fori_loop(0, O_SLOTS // 2, project_rest, None)
    for i in range(pieces):
        a_copy(i).wait_send()
    for m in range(6):
        for part in range(2):

            @pl.when(among(c, SENDS[m][part]))
            def _():
                for copy in out[m][part]:
                    copy.wait_send()

    for g in range(1, kvh):
        o_copy(jnp.int32(g)).wait_send()

    @pl.when(late)
    def _():
        q_copy.wait_send()

    @pl.when(jnp.logical_not(late))
    def _():
        o_copy(jnp.int32(0)).wait_send()
        for copy in g_copies():
            copy.wait_send()


def solution(mesh):
    chips = mesh.shape["sp"] // CORES

    def step(x, gain, wq, wk, wv, wo):
        own, width = x.shape
        shared = own * CORES
        kvh = wk.shape[1] // HEAD // CORES
        heads = wq.shape[1] // HEAD // CORES
        group = heads // kvh
        bf16, f32 = jnp.bfloat16, jnp.float32
        dma, pieces = pltpu.SemaphoreType.DMA, 4
        return pl.pallas_call(
            functools.partial(kernel, chips),
            out_shape=pltpu.VMEM((own, width), bf16),
            in_specs=[pl.BlockSpec(memory_space=pl.ANY)] * 6,
            out_specs=pl.BlockSpec(memory_space=pltpu.VMEM),
            scratch_shapes=[
                pltpu.VMEM((shared, width), bf16),
                pltpu.VMEM((SLOTS * width, WIDE), bf16),
                pltpu.VMEM((width,), bf16),
                pltpu.VMEM((2, shared, HEAD), f32),
                pltpu.VMEM((shared, WIDE), bf16),
                pltpu.VMEM((shared, WIDE), bf16),
                pltpu.VMEM((heads, CORES, 2 * HEAD, own), bf16),
                pltpu.VMEM((group + 2, CORES, HEAD, own), bf16),
                pltpu.VMEM((group, CORES, HEAD, own), bf16),
                pltpu.VMEM((chips, CORES, kvh, own, HEAD), bf16),
                pltpu.VMEM((chips, CORES, kvh, HEAD + ONES, own), bf16),
                pltpu.VMEM((heads * CORES * (HEAD + ONES), own), f32),
                pltpu.VMEM((heads * CORES, 1, own), f32),
                pltpu.VMEM((CORES + 1, own, heads * HEAD), bf16),
                pltpu.VMEM((CORES, own, group * HEAD), bf16),
                dma((pieces,)), dma, dma((O_SLOTS, 2 * kvh)), dma((pieces,)), dma((pieces,)), dma((6, 2, 2)), dma((6, 2, 2)), dma, dma, dma((kvh,)), dma((kvh,)),
                dma((CORES,)), dma((CORES,)),
            ],
            compiler_params=pltpu.CompilerParams(collective_id=0, has_side_effects=True, vmem_limit_bytes=60 * 2**20),
        )(x, gain, wq, wk, wv, wo)

    tokens, whole = P(("dp", "sp"), None), P(None, None)
    return jax.shard_map(
        step,
        mesh=mesh,
        in_specs=(tokens, P(None), whole, whole, whole, whole),
        out_specs=tokens,
        check_vma=False,
    )
```
